32 devices in a mesh: ctx: 16 (over z, x, core), head: 2 (over y).
Axes of the slice: x: 2, y: 2, z: 4, core: 2. Of those that a mesh axis runs over, the one named last changes fastest.
Arguments:
- queries: bfloat16 [8192, 4096], P('ctx', 'head'), may hold values from -10 to 10
- key_states: bfloat16 [8192, 1024], P('ctx', 'head'), may hold values from -10 to 10
- value_rows_stored: bfloat16 [8192, 1024], P('ctx', 'head'), may hold values from -6 to 6
- span_order: int32 [16, 4], replicated, may hold values from 0 to 3, each once within a row
- doc_lengths: int32 [16], replicated, may hold values from 1 to 1792, 8192 in all
- w_out: bfloat16 [4096, 4096], P('ctx', 'head'), may hold values from -0.09375 to 0.09375
Outputs:
- projected: bfloat16 [8192, 4096], P('ctx', 'head')
The draws below stay inside these ranges and needn't reach their ends.
Inputs may be any that keep to these rules, and one draw needn't show every extreme that they name: `span_order`: each row is a permutation of 0 to 3, so each shard holds the 4 spans of its own 512 consecutive positions in some order. `doc_lengths`: the lengths sum to 8192; the longest is exactly 1792.
All inputs are finite; a program needn't handle non-finite values.
Results may differ from the reference program's by a relative error of at most 0.0055.
Values may be sent and summed in bfloat16 or wider, within the bound.
No kernel may reach another device: no remote copies, remote signals or barrier semaphores. Data moves between devices by JAX's collectives and lax.ppermute only.
A program may use at most 128 MiB of HBM per device.

```python
import math
import jax
import jax.numpy as jnp
import numpy as np
from jax import lax

QUERY_HEADS = 32
KEY_VALUE_HEADS = 8
HEAD_SIZE = 128
D = 4096
SHARD_TOKENS = 512
BLK = 128
PACKED_TOKENS = 8192
CPS = 4
MOST_DOC = 1792
DOCS = 16
REACH = 4
N_CTX = 16


def draw_queries(key, part):
    base_offset = jax.random.fold_in(key, 5)
    gathered_values = jax.random.truncated_normal(base_offset, -6.0, 6.0, (PACKED_TOKENS, QUERY_HEADS * HEAD_SIZE))
    return gathered_values.astype(jnp.bfloat16)


def draw_key_states(key, part):
    base_offset = jax.random.fold_in(key, 9)
    gathered_values = jax.random.truncated_normal(base_offset, -6.0, 6.0, (PACKED_TOKENS, KEY_VALUE_HEADS * HEAD_SIZE))
    return gathered_values.astype(jnp.bfloat16)


def block_scale(rng, extent, cuts, low, high):
    gain, own = 1.0, jax.random.fold_in(rng, 6)
    for axis_at, parts in cuts:
        steps = jnp.exp(jax.random.uniform(jax.random.fold_in(own, axis_at), (parts,), jnp.float32, low / len(cuts), high / len(cuts)))
        gain = gain * jnp.repeat(steps, extent[axis_at] // parts).reshape([-1 if axis == axis_at else 1 for axis in range(len(extent))])
    return gain


def split_up(count, total, reach, skew):
    portions = [(1 << 20) // math.isqrt(standing ** skew) + 1 for standing in range(2, count + 1)]
    surplus, counts = total - reach - (count - 1), [1] * (count - 1)
    while surplus > 0:
        candidates = [i for i in range(count - 1) if counts[i] < reach]
        whole, budget = sum([portions[i] for i in candidates]), surplus
        for i in candidates:
            extra = min(reach - counts[i], max(1, budget * portions[i] // whole), surplus)
            counts[i] = counts[i] + extra
            surplus = surplus - extra
    return np.array([reach] + counts)


def uneven_parts(key, count, total, most, lean):
    if count == 2:
        one = jax.random.randint(key, (), max(1, total - most), min(most, total - 1) + 1)
        return jnp.stack([one, total - one])
    sizes = jnp.asarray(split_up(count, total, most, lean), jnp.int32)
    twos = (count - 1) // 2
    donor, sink = sizes[1:1 + 2 * twos:2], sizes[2:2 + 2 * twos:2]
    room = jnp.minimum(donor - 1, most - sink)
    shifted = jax.random.randint(jax.random.fold_in(key, 1), (twos,), 0, 1 << 20) % (room + 1)
    sizes = sizes.at[1:1 + 2 * twos:2].set(donor - shifted).at[2:2 + 2 * twos:2].set(sink + shifted)
    return sizes[jax.random.permutation(jax.random.fold_in(key, 2), count)]


def bell_draw(own_key, shape, spread, limit, pieces=(), kind=jnp.bfloat16):
    level = block_scale(own_key, shape, pieces, -0.22, 0.18) if pieces else 1.0
    values = jax.random.normal(own_key, shape, jnp.float32) * spread * level
    return jnp.minimum(jnp.maximum(values, -limit), limit).astype(kind)


def setup_inputs(seed: int = 0) -> dict:
    streams_of = jax.random.split(jax.random.key(seed), 7)
    queries = draw_queries(jax.random.fold_in(streams_of[6], 71), 0)
    key_states = draw_key_states(jax.random.fold_in(streams_of[6], 71), 0)
    value_rows_stored = bell_draw(streams_of[2], (PACKED_TOKENS, KEY_VALUE_HEADS * HEAD_SIZE), 1.0, 6.0, ((0, 16), (1, 2)))
    span_order = jax.vmap(lambda own: jax.random.permutation(own, CPS))(jax.random.split(streams_of[3], N_CTX)).reshape((N_CTX, CPS)).astype(jnp.int32)
    doc_lengths = uneven_parts(streams_of[4], DOCS, PACKED_TOKENS, MOST_DOC, 2).astype(jnp.int32)
    w_out = bell_draw(streams_of[5], (QUERY_HEADS * HEAD_SIZE, D), (QUERY_HEADS * HEAD_SIZE) ** -0.5, 0.09375, ((0, 16), (1, 2)))
    return dict(queries=queries, key_states=key_states, value_rows_stored=value_rows_stored, span_order=span_order, doc_lengths=doc_lengths, w_out=w_out)


def stored_positions(span_order):
    stored = jnp.arange(PACKED_TOKENS, dtype=jnp.int32)
    shard_index = stored // SHARD_TOKENS
    slot_index = stored % SHARD_TOKENS // BLK
    return shard_index * SHARD_TOKENS + span_order[shard_index, slot_index].astype(jnp.int32) * BLK + stored % BLK

def reference(queries, key_states, value_rows_stored, span_order, doc_lengths, w_out):
    positions = stored_positions(span_order)
    inverse = jnp.zeros((PACKED_TOKENS,), jnp.int32).at[positions].set(jnp.arange(PACKED_TOKENS, dtype=jnp.int32))
    ordered_q = queries[inverse]
    sorted_keys = key_states[inverse]
    sorted_values = value_rows_stored[inverse]
    ends = jnp.cumsum(doc_lengths).astype(jnp.int32)
    sequence = jnp.arange(PACKED_TOKENS, dtype=jnp.int32)
    doc_ids = jnp.searchsorted(ends, sequence, side='right').astype(jnp.int32)
    visible_window = REACH * SHARD_TOKENS
    queries_per_group = QUERY_HEADS // KEY_VALUE_HEADS
    padded_keys = jnp.concatenate([jnp.zeros((visible_window, KEY_VALUE_HEADS * HEAD_SIZE), jnp.bfloat16), sorted_keys], axis=0)
    padded_values = jnp.concatenate([jnp.zeros((visible_window, KEY_VALUE_HEADS * HEAD_SIZE), jnp.bfloat16), sorted_values], axis=0)
    pad_docs = jnp.concatenate([jnp.full((visible_window,), -1, jnp.int32), doc_ids], axis=0)

    def block(index):
        start = index * SHARD_TOKENS
        query_tile_rows = lax.dynamic_slice_in_dim(ordered_q, start, SHARD_TOKENS, 0).astype(jnp.float32)
        query_tile_rows = query_tile_rows.reshape(SHARD_TOKENS, KEY_VALUE_HEADS, queries_per_group, HEAD_SIZE)
        key_tile_rows = lax.dynamic_slice_in_dim(padded_keys, start, visible_window + SHARD_TOKENS, 0).astype(jnp.float32)
        key_tile_rows = key_tile_rows.reshape(visible_window + SHARD_TOKENS, KEY_VALUE_HEADS, HEAD_SIZE)
        value_tile_rows = lax.dynamic_slice_in_dim(padded_values, start, visible_window + SHARD_TOKENS, 0).astype(jnp.float32)
        value_tile_rows = value_tile_rows.reshape(visible_window + SHARD_TOKENS, KEY_VALUE_HEADS, HEAD_SIZE)
        key_docs = lax.dynamic_slice_in_dim(pad_docs, start, visible_window + SHARD_TOKENS, 0)
        key_pos = start - visible_window + jnp.arange(visible_window + SHARD_TOKENS, dtype=jnp.int32)
        query_pos = start + jnp.arange(SHARD_TOKENS, dtype=jnp.int32)
        query_docs = lax.dynamic_slice_in_dim(doc_ids, start, SHARD_TOKENS, 0)
        visible = (query_docs[:, None] == key_docs[None, :]) & (key_pos[None, :] <= query_pos[:, None])
        scores = jnp.einsum('qhgd,khd->hgqk', query_tile_rows, key_tile_rows) / math.sqrt(HEAD_SIZE)
        masked = jnp.where(visible[None, None], scores, -1e+30)
        peak = lax.optimization_barrier(jnp.max(masked, axis=-1, keepdims=True))
        weights = jnp.where(visible[None, None], jnp.exp(masked - peak), 0.0)
        totals = lax.optimization_barrier(jnp.sum(weights, axis=-1))
        rounded = lax.optimization_barrier(weights.astype(jnp.bfloat16)).astype(jnp.float32)
        accum = jnp.einsum('hgqk,khd->hgqd', rounded, value_tile_rows)
        result = accum / totals[..., None]
        return result.transpose(2, 0, 1, 3).reshape(SHARD_TOKENS, QUERY_HEADS * HEAD_SIZE).astype(jnp.bfloat16)
    attended = lax.map(block, jnp.arange(PACKED_TOKENS // SHARD_TOKENS, dtype=jnp.int32)).reshape(PACKED_TOKENS, QUERY_HEADS * HEAD_SIZE)
    stored_rows = attended[positions]
    product = jnp.dot(stored_rows.astype(jnp.float32), w_out.astype(jnp.float32), preferred_element_type=jnp.float32)
    return product.astype(jnp.bfloat16)
```

```python
import functools
import math

import jax
import jax.numpy as jnp
from jax import lax
from jax.experimental import pallas as pl
from jax.experimental.pallas import tpu as pltpu
from jax.sharding import PartitionSpec as P

HEAD_SIZE = 128
BLK = 128
FAR = 1 << 30
NEG = -1e30


def attend_kernel(
    heads, group, slots, table, queries, low_minus_lane, *refs
):
    buffers = refs[: slots // 4]
    out, held, stacked, scores, peak, total, accum, picked, picked_pos, sems = refs[slots // 4 :]
    rows = group * BLK
    copies = []
    for index, buffer in enumerate(buffers):
        span = buffer.shape[0]
        copies.append(
            pltpu.make_async_copy(buffer, held.at[pl.ds(index * span, span)], sems.at[index])
        )
        copies[-1].start()
    for copy in copies:
        copy.wait()
    constant = math.log2(math.e) / math.sqrt(HEAD_SIZE)
    lane = lax.broadcasted_iota(jnp.int32, (BLK, BLK), 1)
    row = lax.broadcasted_iota(jnp.int32, (BLK, BLK), 0)

    @pl.loop(0, queries.shape[0] // BLK)
    def per_block(block):
        q_pos = table[slots + block]
        low_first = table[slots + 4 + block]
        low_last = table[slots + 8 + block]
        q_rows = pl.ds(pl.multiple_of(block * BLK, BLK), BLK)

        def look(slot, count):
            k_pos = table[slot]
            picked[count] = slot
            picked_pos[count] = k_pos
            live = (k_pos <= q_pos) & (k_pos + (BLK - 1) >= low_first)
            return count + live.astype(jnp.int32)

        count = lax.fori_loop(0, slots, look, 0)
        picked[count] = 0
        picked_pos[count] = FAR
        pairs = (count + 1) // 2
        for h in range(heads):
            for j in range(group):
                col = (h * group + j) * HEAD_SIZE
                stacked[h, j * BLK : (j + 1) * BLK, :] = queries[q_rows, col : col + HEAD_SIZE]
            peak[h] = jnp.full((rows, BLK), NEG, jnp.float32)
            total[h] = jnp.zeros((rows, BLK), jnp.float32)
            accum[h] = jnp.zeros((rows, HEAD_SIZE), jnp.float32)
        upper = q_pos + row - lane
        lower = low_minus_lane[q_rows, :]

        def two(pair, col):
            first = pl.ds(pl.multiple_of(picked[2 * pair] * BLK, BLK), BLK)
            second = pl.ds(pl.multiple_of(picked[2 * pair + 1] * BLK, BLK), BLK)
            cols = slice(col, col + HEAD_SIZE)
            return jnp.concatenate([held[first, cols], held[second, cols]], axis=0)

        def products(pair, h):
            return lax.dot_general(
                stacked[h],
                two(pair, h * HEAD_SIZE),
                (((1,), (1,)), ((), ())),
                preferred_element_type=jnp.float32,
            )

        @pl.loop(0, pairs)
        def score(pair):
            pos_a = picked_pos[2 * pair]
            pos_b = picked_pos[2 * pair + 1]
            whole = (
                (pos_a + BLK <= q_pos + 1)
                & (pos_b + BLK <= q_pos + 1)
                & (pos_a >= low_last)
                & (pos_b >= low_last)
            )

            @pl.when(whole)
            def _():
                for h in range(heads):
                    value = products(pair, h)
                    scores[pair, h] = value
                    peak[h] = jnp.maximum(
                        peak[h], jnp.maximum(value[:, :BLK], value[:, BLK:])
                    )

            @pl.when(jnp.logical_not(whole))
            def _():
                seen_a = (upper >= pos_a) & (lower <= pos_a)
                seen_b = (upper >= pos_b) & (lower <= pos_b)
                for h in range(heads):
                    value = products(pair, h)
                    for j in range(group):
                        part = slice(j * BLK, (j + 1) * BLK)
                        left = jnp.where(seen_a, value[part, :BLK], NEG)
                        right = jnp.where(seen_b, value[part, BLK:], NEG)
                        scores[pair, h, part, :BLK] = left
                        scores[pair, h, part, BLK:] = right
                        peak[h, part, :] = jnp.maximum(
                            peak[h, part, :], jnp.maximum(left, right)
                        )

        for h in range(heads):
            top = jnp.max(peak[h], axis=1, keepdims=True) * constant
            peak[h] = jnp.broadcast_to(top, (rows, BLK))

        @pl.loop(0, pairs)
        def weigh(pair):
            for h in range(heads):
                top = peak[h]
                left = jnp.exp2(scores[pair, h, :, :BLK] * constant - top)
                right = jnp.exp2(scores[pair, h, :, BLK:] * constant - top)
                total[h] += left + right
                weights = jnp.concatenate([left, right], axis=1).astype(jnp.bfloat16)
                accum[h] += jnp.dot(
                    weights,
                    two(pair, (heads + h) * HEAD_SIZE),
                    preferred_element_type=jnp.float32,
                )

        for h in range(heads):
            inverse = 1.0 / jnp.sum(total[h], axis=1, keepdims=True)
            result = (accum[h] * inverse).astype(jnp.bfloat16)
            for j in range(group):
                col = (h * group + j) * HEAD_SIZE
                out[q_rows, col : col + HEAD_SIZE] = result[j * BLK : (j + 1) * BLK, :]


def attend(table, queries, part, parts, low_minus_lane, buffers):
    rows, width = queries.shape
    width //= parts
    heads = buffers[0].shape[1] // (2 * HEAD_SIZE)
    group = width // (heads * HEAD_SIZE)
    slots = 4 * len(buffers)
    whole = pl.BlockSpec(memory_space=pl.ANY)
    stack = group * BLK
    return pl.pallas_call(
        functools.partial(attend_kernel, heads, group, slots),
        out_shape=jax.ShapeDtypeStruct((rows, width), jnp.bfloat16),
        grid_spec=pltpu.PrefetchScalarGridSpec(
            num_scalar_prefetch=1,
            grid=(1,),
            in_specs=[
                pl.BlockSpec((rows, width), lambda i, t: (0, part)),
                pl.BlockSpec((rows, BLK), lambda i, t: (0, 0)),
            ]
            + [whole] * len(buffers),
            out_specs=pl.BlockSpec((rows, width), lambda i, t: (0, 0)),
            scratch_shapes=[
                pltpu.VMEM((slots * BLK, buffers[0].shape[1]), jnp.bfloat16),
                pltpu.VMEM((heads, stack, HEAD_SIZE), jnp.bfloat16),
                pltpu.VMEM((slots // 2, heads, stack, 2 * BLK), jnp.float32),
                pltpu.VMEM((heads, stack, BLK), jnp.float32),
                pltpu.VMEM((heads, stack, BLK), jnp.float32),
                pltpu.VMEM((heads, stack, HEAD_SIZE), jnp.float32),
                pltpu.SMEM((slots + 2,), jnp.int32),
                pltpu.SMEM((slots + 2,), jnp.int32),
                pltpu.SemaphoreType.DMA((len(buffers),)),
            ],
        ),
        cost_estimate=pl.CostEstimate(
            flops=4 * rows * width * 4 * rows, bytes_accessed=rows * width * 12, transcendentals=0
        ),
        name="attend",
    )(table, queries, low_minus_lane, *buffers)


def moved(array, axis, pairs):
    return lax.ppermute(array, axis, pairs)


def per_device(queries, key_states, value_rows_stored, span_order, doc_lengths, w_out):
    me = lax.axis_index("ctx")
    size = lax.axis_size("ctx")
    rows = queries.shape[0]
    kv_width = key_states.shape[1]
    parts = 2
    half = kv_width // parts
    layer = 4
    up = [(i, i + layer) for i in range(size - layer)]
    across = [(i, i ^ 2) for i in range(size)]
    partner = [(i, i ^ 1) for i in range(size)]
    is_right = (me // 2) % 2 == 1

    own = [
        jnp.concatenate(
            [key_states[:, p * half : (p + 1) * half], value_rows_stored[:, p * half : (p + 1) * half]],
            axis=1,
        )
        for p in range(parts)
    ]
    held = []
    for p in range(parts):
        own_p = moved(own[p], "ctx", partner)
        lower = moved(own[p], "ctx", up)
        side = moved(jnp.where(is_right, lower, own[p]), "ctx", across)
        held.append(
            [own[p], own_p, lower, moved(lower, "ctx", partner), side, moved(side, "ctx", partner)]
        )
    other = me ^ 1
    shards = jnp.stack([me, other, me - layer, other - layer, me - 2, other - 2])
    order = span_order[jnp.clip(shards, 0, size - 1)]
    spans = shards[:, None] * rows + order * BLK
    spans = jnp.where(shards[:, None] >= 0, spans, FAR).reshape(-1)
    ends = jnp.cumsum(doc_lengths)
    starts = ends - doc_lengths
    q_spans = spans[:4]

    def low(positions):
        at = positions[..., None]
        return jnp.max(jnp.where(starts <= at, starts, 0), axis=-1)

    table = jnp.concatenate([spans, q_spans, low(q_spans), low(q_spans + BLK - 1)]).astype(jnp.int32)
    q_pos = (q_spans[:, None] + jnp.arange(BLK, dtype=jnp.int32)).reshape(-1)
    low_minus_lane = low(q_pos)[:, None] - jnp.arange(BLK, dtype=jnp.int32)
    attended = []
    for p in range(parts):
        attended.append(attend(table, queries, p, parts, low_minus_lane, held[p]))
    all_w = lax.all_gather(w_out, "ctx", axis=0, tiled=True)
    mine = jnp.concatenate(attended, axis=1)
    theirs = jnp.concatenate([moved(a, "head", [(0, 1), (1, 0)]) for a in attended], axis=1)
    here = lax.axis_index("head")
    first = jnp.where(here == 0, mine, theirs)
    second = jnp.where(here == 0, theirs, mine)
    all_heads = jnp.concatenate([first, second], axis=1)
    projected = jnp.dot(all_heads, all_w, preferred_element_type=jnp.float32)
    return projected.astype(jnp.bfloat16)


def solution(mesh):
    placed = (P("ctx", "head"), P("ctx", "head"), P("ctx", "head"), P(), P(), P("ctx", "head"))
    return jax.shard_map(
        per_device, mesh=mesh, in_specs=placed, out_specs=P("ctx", "head"), check_vma=False
    )
```
